32 devices in a mesh: grp: 4 (over y, core), dev: 8 (over z, x).
Axes of the slice: x: 2, y: 2, z: 4, core: 2. Of those that a mesh axis runs over, the one named last changes fastest.
Arguments:
- targets: float32 [64, 16384], P(None, ('grp', 'dev')), may hold values from -1.7 to 1.7
- source_grid: int32 [64, 4096], P(None, ('grp', 'dev')), may hold values from -1331000 to 1331000
- source_weight: int32 [1, 4096], P(None, ('grp', 'dev')), may hold values from 1 to 1024
Outputs:
- kernel_sum: float32 [16384], P(('grp', 'dev'))
The draws below stay inside these ranges and needn't reach their ends.
All inputs are finite; a program needn't handle non-finite values.
Results may differ from the reference program's by a relative error of at most 0.00017.
Values sent between devices are 32-bit elements; how exact they have to be, the bound alone decides.
A program may use at most 64 MiB of HBM per device.

```python
import jax
import jax.numpy as jnp
from jax import lax

D = 64
TGT_DEV = 512
SRC_DEV = 128
TARGETS = 16384
SOURCES = 4096
N_DEV = 8


def centre_table(key):
    centre_count = max(SOURCES // SRC_DEV, 1)
    return jax.random.randint(jax.random.fold_in(key, 11), (D, centre_count), -495000, 495001)


def draw_source_grid(key, part):
    centre_count = max(SOURCES // SRC_DEV, 1)
    centres = centre_table(key)
    owner = jax.random.permutation(jax.random.fold_in(key, 12), SOURCES) % centre_count
    first_noise = jax.random.randint(jax.random.fold_in(key, 13), (D, SOURCES), -418000, 418001)
    second_noise = jax.random.randint(jax.random.fold_in(key, 14), (D, SOURCES), -418000, 418001)
    return (centres[:, owner] + first_noise + second_noise).astype(jnp.int32)


def draw_targets(key, part):
    centre_count = max(SOURCES // SRC_DEV, 1)
    centres = centre_table(key).astype(jnp.float32) / 1048576.0
    owner = jax.random.randint(jax.random.fold_in(key, 15), (TARGETS,), 0, centre_count)
    base = centres[:, owner]
    noise = jnp.clip(0.326 * jax.random.normal(jax.random.fold_in(key, 17), (D, TARGETS), jnp.float32), -1.2, 1.2)
    return (base + noise).astype(jnp.float32)


def place_ends(values, key, smallest, top_value):
    index_at = [jax.random.randint(jax.random.fold_in(key, axis), (), 0, length) for axis, length in enumerate(values.shape)]
    widest = values.shape.index(max(values.shape))
    neighbour = index_at[:widest] + [(index_at[widest] + 1) % values.shape[widest]] + index_at[widest + 1:]
    return values.at[tuple(index_at)].set(smallest).at[tuple(neighbour)].set(top_value)


def setup_inputs(seed: int = 0) -> dict:
    arg_keys = jax.random.split(jax.random.key(seed), 4)
    return {
        "targets": draw_targets(jax.random.fold_in(arg_keys[3], 71), 0),
        "source_grid": draw_source_grid(jax.random.fold_in(arg_keys[3], 71), 0),
        "source_weight": place_ends(jax.random.randint(arg_keys[2], (1, SOURCES), 1, 1025), jax.random.fold_in(arg_keys[2], 1), 1, 1024).astype(jnp.int32),
    }


KERNEL_RATE = 0.7


def block_sum(tgt_rows, src_points, src_mass):
    tgt_norm = jnp.sum(tgt_rows * tgt_rows, axis=0)
    src_norm = jnp.sum(src_points * src_points, axis=0)
    inner_prod = lax.dot_general(tgt_rows, src_points, (((0,), (0,)), ((), ())), precision=lax.Precision.HIGHEST, preferred_element_type=jnp.float32)
    distance = tgt_norm[:, None] + src_norm[None, :] - 2.0 * inner_prod
    kernel = jnp.exp(-KERNEL_RATE * distance)
    return jnp.dot(kernel, src_mass[0], precision=lax.Precision.HIGHEST, preferred_element_type=jnp.float32)


def reference(targets, source_grid, source_weight):
    points = source_grid.astype(jnp.float32) / 1048576.0
    masses = source_weight.astype(jnp.float32) / 16.0
    rows_block = TGT_DEV * min(8, N_DEV)
    cols_block = SRC_DEV * 4
    count_cols = SOURCES // cols_block
    point_blocks = jnp.transpose(points.reshape(D, count_cols, cols_block), (1, 0, 2))
    mass_blocks = jnp.transpose(masses.reshape(1, count_cols, cols_block), (1, 0, 2))
    target_blocks = jnp.transpose(targets.reshape(D, TARGETS // rows_block, rows_block), (1, 0, 2))

    def one_target_block(tgt_rows):
        def advance(running, source_pair):
            return running + block_sum(tgt_rows, source_pair[0], source_pair[1]), None
        result, unused = lax.scan(advance, jnp.zeros((rows_block,), jnp.float32), (point_blocks, mass_blocks))
        return result

    sums = lax.map(one_target_block, target_blocks)
    return sums.reshape(TARGETS)
```

```python
import functools
import math

import jax
import jax.numpy as jnp
from jax import lax
from jax.experimental import pallas as pl
from jax.experimental.pallas import tpu as pltpu
from jax.sharding import PartitionSpec as P

KERNEL_RATE = 0.7
RATE = KERNEL_RATE * math.log2(math.e)
GRID_SCALE = 1.0 / 1048576.0
WEIGHT_SCALE = 1.0 / 16.0
EXTRA = 16
VMEM_GRANT = 32 * 1024 * 1024
LANES = 128
MESH = pl.DeviceIdType.MESH


def slot_of(layer, rx, ry):
    return layer * 4 + rx * 2 + ry


def three_parts(value):
    first = value.astype(jnp.bfloat16).astype(jnp.float32)
    rest = value - first
    second = rest.astype(jnp.bfloat16).astype(jnp.float32)
    return first, second, rest - second


def extra_rows(rows, norm, norm_at, ones_at):
    row = lax.broadcasted_iota(jnp.int32, (rows, norm.shape[1]), 0)
    result = jnp.where((row >= ones_at) & (row < ones_at + 3), 1.0, 0.0)
    for i, part in enumerate(three_parts(norm)):
        result = jnp.where(row == norm_at + i, part, result)
    return result


def kernel(
    layers, tgt_hbm, grid_hbm, weight_hbm, out_ref, tgt, slots, lhs, acc, swap, local_sem, send_sem, recv_sem, swap_sem
):
    _, depth, count = tgt.shape
    me_grp, me_dev = lax.axis_index("grp"), lax.axis_index("dev")
    my_y, my_core = me_grp // 2, me_grp % 2
    my_z, my_x = me_dev // 2, me_dev % 2
    along_x = {"grp": me_grp, "dev": my_z * 2 + (1 - my_x)}
    along_y = {"grp": (1 - my_y) * 2 + my_core, "dev": me_dev}
    diagonal = {"grp": (1 - my_y) * 2 + my_core, "dev": my_z * 2 + (1 - my_x)}
    diagonal = {"grp": (1 - my_y) * 2 + my_core, "dev": my_z * 2 + (1 - my_x)}
    across = {"grp": my_y * 2 + (1 - my_core), "dev": me_dev}

    below, above = my_z, layers - 1 - my_z
    both = jnp.minimum(below, above)

    def along_z(step):
        return {"grp": me_grp, "dev": ((my_z + step) % layers) * 2 + my_x}

    def origin(j):
        alternate = my_z + ((j + 1) // 2) * (1 if j % 2 else -1)
        onward = jnp.where(above > below, my_z + (j - both), my_z - (j - both))
        return jnp.where(j <= 2 * both, alternate, onward)

    own = [
        pltpu.make_async_copy(grid_hbm, slots.at[4 * my_z, pl.ds(0, depth)], local_sem.at[0]),
        pltpu.make_async_copy(weight_hbm, slots.at[4 * my_z, pl.ds(depth, 1)], local_sem.at[1]),
    ]
    targets_in = pltpu.make_async_copy(tgt_hbm, tgt.at[0], local_sem.at[2])
    for copy in own:
        copy.start()
    targets_in.start()

    barrier = pltpu.get_barrier_semaphore()
    partners = [along_z(step) for step in range(1, layers)] + [along_x, along_y, diagonal, across]
    for partner in partners:
        pl.semaphore_signal(barrier, inc=1, device_id=partner, device_id_type=MESH)
    pl.semaphore_wait(barrier, len(partners))
    for copy in own:
        copy.wait()

    sent = []

    def view(slot):
        return slots.at[slot, pl.ds(0, depth + 1)]

    def send(source, target, device):
        copy = pltpu.make_async_remote_copy(
            src_ref=view(source),
            dst_ref=view(target),
            send_sem=send_sem.at[len(sent)],
            recv_sem=recv_sem.at[target],
            device_id=device,
            device_id_type=MESH,
        )
        copy.start()
        sent.append(copy)

    def arrive(slot):
        pltpu.make_async_copy(view(slot), view(slot), recv_sem.at[slot]).wait()

    layer = [origin(j) for j in range(layers)]
    mine = slot_of(layer[0], 0, 0)
    for step in range(1, layers):
        send(mine, mine, along_z(step))
    send(mine, mine + 2, along_x)
    send(mine, mine + 1, along_y)

    def swap_copy(source, target, i):
        return pltpu.make_async_remote_copy(
            src_ref=source,
            dst_ref=target,
            send_sem=swap_sem.at[2 * i],
            recv_sem=swap_sem.at[2 * i + 1],
            device_id=across,
            device_id_type=MESH,
        )

    targets_in.wait()
    swap_targets = swap_copy(tgt.at[0], tgt.at[1], 0)
    swap_targets.start()
    tail = jnp.zeros((2 * depth - EXTRA, count), jnp.float32)
    for which in range(2):
        if which == 1:
            swap_targets.wait()
        t = tgt[which]
        norm = jnp.sum(t * t, axis=0, keepdims=True) * (-RATE)
        t1, t2, t3 = three_parts(t * (2.0 * RATE))
        ext = extra_rows(EXTRA, norm, 0, 3)
        for i, pair in enumerate(((t1, t2), (t3, t1), (t2, t1), (ext, tail))):
            block = jnp.concatenate(pair, axis=0)
            lhs[which, :, 2 * depth * i : 2 * depth * (i + 1)] = block.T.astype(jnp.bfloat16)
    acc[...] = jnp.zeros_like(acc)

    def forward(j, rx, ry):
        slot = slot_of(layer[j], rx, ry)
        arrive(slot)
        if rx == 0 and ry == 0:
            send(slot, slot + 2, along_x)
            send(slot, slot + 1, along_y)
            if j > 0:
                send(slot, slot + 3, diagonal)
        elif j > 0:
            pass
        elif rx == 1 and ry == 0 and j % 2 == 0:
            send(slot, slot + 1, along_y)
        elif rx == 0 and ry == 1 and j % 2 == 1:
            send(slot, slot + 2, along_x)

    def source_side(pair):
        blocks = jnp.concatenate([slots[slot_of(layer[j], rx, ry)] for j, rx, ry in pair], axis=1)
        p = blocks[:depth].astype(jnp.float32) * GRID_SCALE
        mass = blocks[depth : depth + 1].astype(jnp.float32) * WEIGHT_SCALE
        p_norm = jnp.sum(p * p, axis=0, keepdims=True) * (-RATE)
        p1, p2, p3 = three_parts(p)
        p_ext = extra_rows(EXTRA, p_norm, 3, 0)
        p_tail = jnp.zeros((2 * depth - EXTRA, p.shape[1]), jnp.float32)
        return jnp.concatenate([p1, p1, p1, p2, p2, p3, p_ext, p_tail], axis=0).astype(jnp.bfloat16), mass

    def add_terms(which, rhs, mass):
        terms = jnp.exp2(jnp.dot(lhs[which], rhs, preferred_element_type=jnp.float32)) * mass
        total = acc[which]
        for i in range(terms.shape[1] // LANES):
            total = total + terms[:, i * LANES : (i + 1) * LANES]
        acc[which] = total

    def compute(pair):
        side = source_side(pair)
        add_terms(1, *side)
        add_terms(0, *side)

    def reduced(which):
        return jnp.sum(acc[which].T, axis=0, keepdims=True)

    far = range(1, layers)
    forward(1, 0, 0)
    forward(0, 1, 0)
    forward(0, 0, 1)
    for j in far[1:]:
        forward(j, 0, 0)
    forward(0, 1, 1)
    ready = [(0, 0, 0), (0, 1, 0), (0, 0, 1)] + [(j, 0, 0) for j in far] + [(0, 1, 1)]
    for j in far:
        forward(j, 1, 0)
        forward(j, 0, 1)
        ready += [(j, 1, 0), (j, 0, 1)]
        for _ in range(min(2, len(ready) // 2)):
            compute(ready[:2])
            ready = ready[2:]
    for j in far:
        while len(ready) > 1:
            compute(ready[:2])
            ready = ready[2:]
        forward(j, 1, 1)
        ready += [(j, 1, 1)]
    while len(ready) > 2:
        compute(ready[:2])
        ready = ready[2:]
    side = source_side(ready)
    add_terms(1, *side)
    swap[0] = reduced(1)
    for copy in sent:
        copy.wait_send()
    swap_sums = swap_copy(swap.at[0], swap.at[1], 1)
    swap_sums.start()
    add_terms(0, *side)
    result = reduced(0)
    swap_sums.wait()
    out_ref[...] = result + swap[1]

def shards(layers, targets, source_grid, source_weight):
    depth, count = targets.shape
    width = source_grid.shape[1]
    slot_count = layers * 4
    copies = slot_count
    result = pl.pallas_call(
        functools.partial(kernel, layers),
        out_shape=jax.ShapeDtypeStruct((1, count), jnp.float32),
        in_specs=[pl.BlockSpec(memory_space=pltpu.HBM)] * 3,
        out_specs=pl.BlockSpec(memory_space=pltpu.VMEM),
        scratch_shapes=[
            pltpu.VMEM((2, depth, count), jnp.float32),
            pltpu.VMEM((slot_count, depth + 8, width), jnp.int32),
            pltpu.VMEM((2, count, 8 * depth), jnp.bfloat16),
            pltpu.VMEM((2, count, LANES), jnp.float32),
            pltpu.VMEM((2, 1, count), jnp.float32),
            pltpu.SemaphoreType.DMA((3,)),
            pltpu.SemaphoreType.DMA((copies,)),
            pltpu.SemaphoreType.DMA((slot_count,)),
            pltpu.SemaphoreType.DMA((4,)),
        ],
        compiler_params=pltpu.CompilerParams(collective_id=0, has_side_effects=True, vmem_limit_bytes=VMEM_GRANT),
    )(*[pltpu.with_memory_space_constraint(a, pltpu.HBM) for a in (targets, source_grid, source_weight)])
    return result.reshape(count)


def solution(mesh):
    layers = mesh.shape["dev"] // 2
    in_specs = (P(None, ("grp", "dev")), P(None, ("grp", "dev")), P(None, ("grp", "dev")))
    out_specs = P(("grp", "dev"))
    return jax.shard_map(
        functools.partial(shards, layers), mesh=mesh, in_specs=in_specs, out_specs=out_specs, check_vma=False
    )
```
